8 devices in a mesh: dp: 1 (over z), tp: 8 (over x, y, core).
Axes of the slice: x: 2, y: 2, z: 1, core: 2. Of those that a mesh axis runs over, the one named last changes fastest.
Arguments:
- x: bfloat16 [2048, 12288], P('dp')
- w_gate: bfloat16 [12288, 33792], P(None, 'tp')
- w_up: bfloat16 [12288, 33792], P(None, 'tp')
- w_down: bfloat16 [33792, 12288], P('tp')
Outputs:
- output: bfloat16 [2048, 12288], P('dp')
All inputs are finite; a program needn't handle non-finite values.
Results may differ from the reference program's by a relative error of at most 0.016.
Values are sent between devices in bfloat16 or wider.
A program may use at most 2 GiB of HBM per device.

```python
import jax
import jax.numpy as jnp

ROWS = 2048
D = 12288
FF = 33792


def setup_inputs(seed: int = 0, part: int = 0) -> dict:
    kx, kg, ku, kd = jax.random.split(jax.random.key(seed), 4)
    drawn = {
        "x": jax.random.normal(jax.random.fold_in(kx, part), (ROWS, D), jnp.float32),
        "w_gate": jax.random.normal(kg, (D, FF), jnp.float32) * D**-0.5,
        "w_up": jax.random.normal(ku, (D, FF), jnp.float32) * D**-0.5,
        "w_down": jax.random.normal(kd, (FF, D), jnp.float32) * FF**-0.5,
    }
    return {k: v.astype(jnp.bfloat16) for k, v in drawn.items()}


def reference(x, w_gate, w_up, w_down):
    gate = jnp.dot(x, w_gate, preferred_element_type=jnp.float32)
    up = jnp.dot(x, w_up, preferred_element_type=jnp.float32)
    hidden = (jax.nn.silu(gate) * up).astype(jnp.bfloat16)
    return jnp.dot(hidden, w_down, preferred_element_type=jnp.float32).astype(jnp.bfloat16)
```

```python
import functools

import jax
import jax.numpy as jnp
from jax import lax
from jax.experimental import pallas as pl
from jax.experimental.pallas import tpu as pltpu
from jax.sharding import PartitionSpec as P

MESH = pl.DeviceIdType.MESH
F32, BF16 = jnp.float32, jnp.bfloat16

BM = 512
GC = 128
DC = 1024
NB = 4
H0, H1, H2 = BM // 2, BM // 4, BM // 8


def kernel(x_hbm, wg_hbm, wu_hbm, wd_hbm, y_hbm, x_v, w_v, h_v, d_v, keep, out0, in0, out1, in1, out2, in2, fin,
           x_sem, w_sem, d_sem, s_sem, r_sem, f_sem):
    rows, ff = x_hbm.shape[0], wg_hbm.shape[1]
    chunks, ng, nd = rows // BM, ff // GC, y_hbm.shape[1] // DC
    tiles, gates = chunks * nd, chunks * ng

    me = lax.axis_index("tp")
    core, cy, cx = me % 2, (me // 2) % 2, me // 4
    partner = me + 1 - 2 * core
    ny, nx = me + 2 - 4 * cy, me + 4 - 8 * cx

    def x_load(c):
        return pltpu.make_async_copy(x_hbm.at[pl.ds(c * BM, BM)], x_v, x_sem)

    def w_load(i):
        slot = i % 2
        cols = pl.ds(pl.multiple_of((i % ng) * GC, GC), GC)
        return (
            pltpu.make_async_copy(wg_hbm.at[:, cols], w_v.at[slot, :, pl.ds(0, GC)], w_sem.at[slot, 0]),
            pltpu.make_async_copy(wu_hbm.at[:, cols], w_v.at[slot, :, pl.ds(GC, GC)], w_sem.at[slot, 1]),
        )

    def d_load(t):
        slot = t % 2
        cols = pl.ds(pl.multiple_of((t % nd) * DC, DC), DC)
        return pltpu.make_async_copy(wd_hbm.at[:, cols], d_v.at[slot], d_sem.at[slot])

    def place(t):
        turn = t % 2
        first = cx * (1 - turn) + cy * turn
        second = cy * (1 - turn) + cx * turn
        n1 = nx * (1 - turn) + ny * turn
        n2 = ny * (1 - turn) + nx * turn
        return t % NB, first, second, n1, n2

    def remote(src, dst, stage, slot, to):
        return pltpu.make_async_remote_copy(
            src_ref=src, dst_ref=dst, send_sem=s_sem.at[stage, slot], recv_sem=r_sem.at[stage, slot],
            device_id={"tp": to}, device_id_type=MESH,
        )

    def y_at(t, offset, size):
        row = (t // nd) * BM + offset
        return y_hbm.at[pl.ds(pl.multiple_of(row, size), size), pl.ds(pl.multiple_of((t % nd) * DC, DC), DC)]

    def send(t, stage):
        slot, first, second, n1, n2 = place(t)
        if stage == 0:
            return remote(out0.at[slot], in0.at[slot], 0, slot, partner)
        if stage == 1:
            return remote(out1.at[slot], in1.at[slot], 1, slot, n1)
        if stage == 2:
            return remote(out2.at[slot], in2.at[slot], 2, slot, n2)
        if stage == 3:
            block = y_at(t, core * H0 + first * H1 + second * H2, H2)
            return remote(fin.at[slot], block, 3, slot, n2)
        if stage == 4:
            block = y_at(t, core * H0 + first * H1, H1)
            return remote(block, block, 4, slot, n1)
        block = y_at(t, core * H0, H0)
        return remote(block, block, 5, slot, partner)

    def own(t):
        slot, first, second, _, _ = place(t)
        return pltpu.make_async_copy(fin.at[slot], y_at(t, core * H0 + first * H1 + second * H2, H2), f_sem.at[slot])

    def at(base, size):
        return pl.ds(pl.multiple_of(base, size), size)

    def advance(t, n):
        slot, first, second, _, _ = place(t)
        send(t, n - 1).wait()
        if n == 1:
            mine, theirs = at(first * H1, H1), at((1 - first) * H1, H1)
            out1[slot] = (keep[slot, theirs, :] + in0[slot, theirs, :].astype(F32)).astype(BF16)
            keep[slot, mine, :] = keep[slot, mine, :] + in0[slot, mine, :].astype(F32)
            send(t, 1).start()
        elif n == 2:
            mine, theirs = at(first * H1 + second * H2, H2), at(first * H1 + (1 - second) * H2, H2)
            out2[slot] = (keep[slot, theirs, :] + in1[slot, at((1 - second) * H2, H2), :].astype(F32)).astype(BF16)
            keep[slot, mine, :] = keep[slot, mine, :] + in1[slot, at(second * H2, H2), :].astype(F32)
            send(t, 2).start()
        elif n == 3:
            mine = at(first * H1 + second * H2, H2)
            fin[slot] = (keep[slot, mine, :] + in2[slot].astype(F32)).astype(BF16)
            send(t, 3).start()
            own(t).start()
        elif n == 4:
            own(t).wait()
            send(t, 4).start()
        elif n == 5:
            send(t, 5).start()

    def tick(t, guard):
        for n in range(6, 0, -1):
            if guard:
                pl.when(t >= n)(functools.partial(advance, t - n, n))
            else:
                advance(t - n, n)

    def gate_step(c, g):
        i = c * ng + g

        @pl.when(g == 0)
        def _():
            x_load(c).wait()

        for copy in w_load(i):
            copy.wait()

        @pl.when(i + 1 < gates)
        def _():
            for copy in w_load(i + 1):
                copy.start()

        both = jnp.dot(x_v[...], w_v[i % 2], preferred_element_type=F32)
        gate, up = both[:, :GC], both[:, GC:]
        h_v[c % 2, :, pl.ds(pl.multiple_of(g * GC, GC), GC)] = (jax.nn.silu(gate) * up).astype(BF16)

        @pl.when((g == ng - 1) & (c + 1 < chunks))
        def _():
            x_load(c + 1).start()

    def down_step(t, guard):
        c, slot = t // nd, t % NB
        d_load(t).wait()

        @pl.when(t + 1 < tiles)
        def _():
            d_load(t + 1).start()

        tick(t, guard)
        theirs, mine = at((1 - core) * H0, H0), at(core * H0, H0)
        out0[slot] = jnp.dot(h_v[c % 2, theirs, :], d_v[t % 2], preferred_element_type=F32).astype(BF16)
        keep[slot] = jnp.dot(h_v[c % 2, mine, :], d_v[t % 2], preferred_element_type=F32)
        send(t, 0).start()

    x_load(0).start()
    for copy in w_load(0):
        copy.start()
    d_load(0).start()

    barrier = pltpu.get_barrier_semaphore()
    for other in (partner, nx, ny):
        pl.semaphore_signal(barrier, inc=1, device_id={"tp": other}, device_id_type=MESH)
    pl.semaphore_wait(barrier, 3)

    @pl.loop(0, ng)
    def _(g):
        gate_step(0, g)

    @pl.loop(0, tiles - nd)
    def _(t):
        c, d = t // nd + 1, t % nd

        @pl.loop(d * ng // nd, (d + 1) * ng // nd)
        def _(g):
            gate_step(c, g)

        down_step(t, True)

    @pl.loop(tiles - nd, tiles)
    def _(t):
        down_step(t, False)

    for t in range(tiles, tiles + 6):
        for n in range(6, 0, -1):
            if 0 <= t - n < tiles:
                advance(t - n, n)


def solution(mesh):
    def step(x, w_gate, w_up, w_down):
        rows, d = x.shape
        ff = w_gate.shape[1]
        dma = pltpu.SemaphoreType.DMA
        return pl.pallas_call(
            kernel,
            out_shape=jax.ShapeDtypeStruct((rows, d), BF16),
            in_specs=[pl.BlockSpec(memory_space=pl.ANY)] * 4,
            out_specs=pl.BlockSpec(memory_space=pl.ANY),
            scratch_shapes=[
                pltpu.VMEM((BM, d), BF16),
                pltpu.VMEM((2, d, 2 * GC), BF16),
                pltpu.VMEM((2, BM, ff), BF16),
                pltpu.VMEM((2, ff, DC), BF16),
                pltpu.VMEM((NB, H0, DC), F32),
                pltpu.VMEM((NB, H0, DC), BF16),
                pltpu.VMEM((NB, H0, DC), BF16),
                pltpu.VMEM((NB, H1, DC), BF16),
                pltpu.VMEM((NB, H1, DC), BF16),
                pltpu.VMEM((NB, H2, DC), BF16),
                pltpu.VMEM((NB, H2, DC), BF16),
                pltpu.VMEM((NB, H2, DC), BF16),
                dma,
                dma((2, 2)),
                dma((2,)),
                dma((6, NB)),
                dma((6, NB)),
                dma((NB,)),
            ],
            compiler_params=pltpu.CompilerParams(
                collective_id=0, has_side_effects=True, vmem_limit_bytes=67_043_328
            ),
            cost_estimate=pl.CostEstimate(
                flops=6 * rows * d * ff, bytes_accessed=2 * (rows // BM * 3 * d * ff + 4 * rows * d), transcendentals=rows * ff
            ),
            name="mlp",
        )(x, w_gate, w_up, w_down)

    return jax.shard_map(
        step,
        mesh=mesh,
        in_specs=(P("dp", None), P(None, "tp"), P(None, "tp"), P("tp", None)),
        out_specs=P("dp", None),
        check_vma=False,
    )
```

```python
import functools

import jax
import jax.numpy as jnp
from jax import lax
from jax.experimental import pallas as pl
from jax.experimental.pallas import tpu as pltpu
from jax.sharding import PartitionSpec as P

MESH = pl.DeviceIdType.MESH
F32, BF16 = jnp.float32, jnp.bfloat16

TM, GC, DC = 256, 128, 768
BM = 2 * TM
NB = 8
NW = 3
H0, H1, H2 = TM // 2, TM // 4, TM // 8


def kernel(x_hbm, wg_hbm, wu_hbm, wd_hbm, y_hbm, x_v, w_v, h_v, d_v, keep, out0, in0, out1, in1, out2, in2, fin,
           x_sem, w_sem, d_sem, s_sem, r_sem, f_sem):
    rows, ff = x_hbm.shape[0], wg_hbm.shape[1]
    ng, nd = ff // GC, y_hbm.shape[1] // DC
    wide = (rows - 2 * TM) // BM
    gates, downs = (wide + 2) * ng, (wide + 2) * nd
    edge, tiles = nd * (1 + 2 * wide), nd * (2 + 2 * wide)

    me = lax.axis_index("tp")
    core, cy, cx = me % 2, (me // 2) % 2, me // 4
    partner = me + 1 - 2 * core
    ny, nx = me + 2 - 4 * cy, me + 4 - 8 * cx

    def at(base, size):
        return pl.ds(pl.multiple_of(base, size), size)

    def x_load(c, size):
        base = jnp.where(c == 0, 0, TM + (c - 1) * BM)
        return pltpu.make_async_copy(x_hbm.at[at(base, TM) if size == TM else pl.ds(pl.multiple_of(base, TM), BM)],
                                     x_v.at[pl.ds(0, size)], x_sem)

    def w_load(i):
        slot = i % NW
        cols = at((i % ng) * GC, GC)
        return (
            pltpu.make_async_copy(wg_hbm.at[:, cols], w_v.at[slot, :, pl.ds(0, GC)], w_sem.at[slot, 0]),
            pltpu.make_async_copy(wu_hbm.at[:, cols], w_v.at[slot, :, pl.ds(GC, GC)], w_sem.at[slot, 1]),
        )

    def d_load(t):
        slot = t % 2
        return pltpu.make_async_copy(wd_hbm.at[:, at((t % nd) * DC, DC)], d_v.at[slot], d_sem.at[slot])

    def place(u):
        turn = u % 2
        first = cx * (1 - turn) + cy * turn
        second = cy * (1 - turn) + cx * turn
        n1 = nx * (1 - turn) + ny * turn
        n2 = ny * (1 - turn) + nx * turn
        return u % NB, first, second, n1, n2

    def remote(src, dst, stage, slot, to):
        return pltpu.make_async_remote_copy(
            src_ref=src, dst_ref=dst, send_sem=s_sem.at[stage, slot], recv_sem=r_sem.at[stage, slot],
            device_id={"tp": to}, device_id_type=MESH,
        )

    def y_at(u, offset, size):
        v = jnp.clip(u - nd, 0, 2 * wide * nd - 1)
        t = v // 2
        row = jnp.where(u < nd, 0, jnp.where(u >= edge, rows - TM, TM + (t // nd) * BM + (v % 2) * TM))
        col = jnp.where((u < nd) | (u >= edge), u % nd, t % nd)
        return y_hbm.at[at(row + offset, size), at(col * DC, DC)]

    def send(u, stage):
        slot, first, second, n1, n2 = place(u)
        if stage == 0:
            return remote(out0.at[slot], in0.at[slot], 0, slot, partner)
        if stage == 1:
            return remote(out1.at[slot], in1.at[slot], 1, slot, n1)
        if stage == 2:
            return remote(out2.at[slot], in2.at[slot], 2, slot, n2)
        if stage == 3:
            block = y_at(u, core * H0 + first * H1 + second * H2, H2)
            return remote(fin.at[slot], block, 3, slot, n2)
        if stage == 4:
            block = y_at(u, core * H0 + first * H1, H1)
            return remote(block, block, 4, slot, n1)
        block = y_at(u, core * H0, H0)
        return remote(block, block, 5, slot, partner)

    def own(u):
        slot, first, second, _, _ = place(u)
        return pltpu.make_async_copy(fin.at[slot], y_at(u, core * H0 + first * H1 + second * H2, H2), f_sem.at[slot])

    def arrived(u, n):
        send(u, n - 1).wait()
        if n == 4:
            own(u).wait()

    def add(u, n):
        slot, first, second, _, _ = place(u)
        if n == 1:
            mine, theirs = at(first * H1, H1), at((1 - first) * H1, H1)
            out1[slot] = (keep[slot, theirs, :] + in0[slot, theirs, :].astype(F32)).astype(BF16)
            keep[slot, mine, :] = keep[slot, mine, :] + in0[slot, mine, :].astype(F32)
        elif n == 2:
            mine, theirs = at(first * H1 + second * H2, H2), at(first * H1 + (1 - second) * H2, H2)
            out2[slot] = (keep[slot, theirs, :] + in1[slot, at((1 - second) * H2, H2), :].astype(F32)).astype(BF16)
            keep[slot, mine, :] = keep[slot, mine, :] + in1[slot, at(second * H2, H2), :].astype(F32)
        elif n == 3:
            mine = at(first * H1 + second * H2, H2)
            fin[slot] = (keep[slot, mine, :] + in2[slot].astype(F32)).astype(BF16)

    def forward(u, n):
        if n < 6:
            send(u, n).start()
        if n == 3:
            own(u).start()

    def tick(u, stages=range(6, 0, -1)):
        for part in (arrived, add, forward):
            for n in stages:
                part(u - 2 * n, n)

    def tick_if(u):
        def one(n):
            for part in (arrived, add, forward):
                part(u - 2 * n, n)

        for n in range(6, 0, -1):
            pl.when(u >= 2 * n)(functools.partial(one, n))

    def gate_step(c, g, size, ticked=None):
        i = c * ng + g

        @pl.when(g == 0)
        def _():
            x_load(c, size).wait()

        for copy in w_load(i):
            copy.wait()

        @pl.when(i + NW - 1 < gates)
        def _():
            for copy in w_load(i + NW - 1):
                copy.start()

        if ticked is not None:
            tick(ticked)
        both = jnp.dot(x_v[pl.ds(0, size), :], w_v[i % NW], preferred_element_type=F32)
        gate, up = both[:, :GC], both[:, GC:]
        h_v[c % 2, pl.ds(0, size), at(g * GC, GC)] = (jax.nn.silu(gate) * up).astype(BF16)

    def down_step(t, c, u, size, before):
        d_load(t).wait()

        @pl.when(t + 1 < downs)
        def _():
            d_load(t + 1).start()

        before()
        for k in range(size // TM):
            slot = (u + k) % NB
            theirs, mine = at(k * TM + (1 - core) * H0, H0), at(k * TM + core * H0, H0)
            out0[slot] = jnp.dot(h_v[c % 2, theirs, :], d_v[t % 2], preferred_element_type=F32).astype(BF16)
            keep[slot] = jnp.dot(h_v[c % 2, mine, :], d_v[t % 2], preferred_element_type=F32)
        for k in range(size // TM):
            send(u + k, 0).start()

    def span(d):
        return d * ng // nd, (d + 1) * ng // nd

    x_load(0, TM).start()
    for i in range(NW - 1):
        for copy in w_load(i):
            copy.start()
    d_load(0).start()

    barrier = pltpu.get_barrier_semaphore()
    for other in (partner, nx, ny):
        pl.semaphore_signal(barrier, inc=1, device_id={"tp": other}, device_id_type=MESH)
    pl.semaphore_wait(barrier, 3)

    @pl.loop(0, ng)
    def _(g):
        gate_step(0, g, TM)

    x_load(1, BM).start()

    @pl.loop(0, nd)
    def _(t):
        down_step(t, 0, t, TM, lambda: tick_if(t))

        @pl.loop(*span(t))
        def _(g):
            gate_step(1, g, BM)

    def group(t, size):
        c, (low, high), u = t // nd, span(t % nd), nd + 2 * (t - nd)
        down_step(t, c, u, BM, lambda: tick(u))
        gate_step(c + 1, low, size, ticked=u + 1)

        @pl.loop(low + 1, high)
        def _(g):
            gate_step(c + 1, g, size)

    x_load(2, BM).start()
    last = wide * nd

    @pl.loop(nd, last)
    def _(t):
        group(t, BM)

        @pl.when((t % nd == nd - 1) & (t < last - 1))
        def _():
            x_load(t // nd + 2, BM).start()

    x_load(wide + 1, TM).start()

    @pl.loop(last, last + nd)
    def _(t):
        group(t, TM)

    @pl.loop(last + nd, downs)
    def _(t):
        u = edge + t - last - nd
        down_step(t, wide + 1, u, TM, lambda: tick(u))

    for u in range(tiles, tiles + 12):
        tick(u, [n for n in range(6, 0, -1) if u - 2 * n < tiles])


def solution(mesh):
    def step(x, w_gate, w_up, w_down):
        rows, d = x.shape
        ff = w_gate.shape[1]
        dma = pltpu.SemaphoreType.DMA
        return pl.pallas_call(
            kernel,
            out_shape=jax.ShapeDtypeStruct((rows, d), BF16),
            in_specs=[pl.BlockSpec(memory_space=pl.ANY)] * 4,
            out_specs=pl.BlockSpec(memory_space=pl.ANY),
            scratch_shapes=[
                pltpu.VMEM((BM, d), BF16),
                pltpu.VMEM((NW, d, 2 * GC), BF16),
                pltpu.VMEM((2, BM, ff), BF16),
                pltpu.VMEM((2, ff, DC), BF16),
                pltpu.VMEM((NB, H0, DC), F32),
                pltpu.VMEM((NB, H0, DC), BF16),
                pltpu.VMEM((NB, H0, DC), BF16),
                pltpu.VMEM((NB, H1, DC), BF16),
                pltpu.VMEM((NB, H1, DC), BF16),
                pltpu.VMEM((NB, H2, DC), BF16),
                pltpu.VMEM((NB, H2, DC), BF16),
                pltpu.VMEM((NB, H2, DC), BF16),
                dma,
                dma((NW, 2)),
                dma((2,)),
                dma((6, NB)),
                dma((6, NB)),
                dma((NB,)),
            ],
            compiler_params=pltpu.CompilerParams(
                collective_id=0, has_side_effects=True, vmem_limit_bytes=67_043_328
            ),
            cost_estimate=pl.CostEstimate(
                flops=6 * rows * d * ff, bytes_accessed=2 * (rows // BM * 3 * d * ff + 4 * rows * d), transcendentals=rows * ff
            ),
            name="mlp",
        )(x, w_gate, w_up, w_down)

    return jax.shard_map(
        step,
        mesh=mesh,
        in_specs=(P("dp", None), P(None, "tp"), P(None, "tp"), P("tp", None)),
        out_specs=P("dp", None),
        check_vma=False,
    )
```
